32 devices in a mesh: freq: 8 (over z, y), pts: 4 (over x, core).
Axes of the slice: x: 2, y: 2, z: 4, core: 2. Of those that a mesh axis runs over, the one named last changes fastest.
Arguments:
- direct: bfloat16 [8, 512, 6144], P('freq', None, 'pts'), may hold values from -6 to 6
- onsets: int32 [8, 6144], P('freq', 'pts'), may hold values from 64 to 511
- left_bases: bfloat16 [128, 24, 24, 2, 8, 256], P('freq', 'pts'), may hold values from -0.4375 to 0.4375
- right_bases: bfloat16 [128, 24, 24, 2, 8, 256], P('freq', 'pts'), may hold values from -0.25 to 0.25
- tile_ranks: int32 [128, 24, 24], P('freq', 'pts'), may hold values from 1 to 8
Outputs:
- plus_field: float32 [8, 512, 6144], P('freq', None, 'pts')
- minus_field: float32 [8, 512, 6144], P('freq', None, 'pts')
The draws below stay inside these ranges and needn't reach their ends.
All inputs are finite; a program needn't handle non-finite values.
Results may differ from the reference program's by a relative error of at most 0.017.
Values may be sent and summed in bfloat16 or wider, within the bound.
A program may use at most 256 MiB of HBM per device.

```python
import math
import jax
import jax.numpy as jnp
from jax import lax

N = 6144
NB = 256
K = 8
F = 128
ITERS = 3
NT = 512
NTL = 24
P_SIZE = 8
N_PTS = 4


def place_ends(drawn, own_key, least, top_value):
    longest = drawn.shape.index(max(drawn.shape))
    spots = []
    for shift in (0, 1):
        where = [jax.random.randint(jax.random.fold_in(own_key, axis), (), 0, length) for axis, length in enumerate(drawn.shape)]
        where[longest] = (where[longest] + shift) % drawn.shape[longest]
        spots.append(tuple(where))
    return drawn.at[spots[0]].set(least).at[spots[1]].set(top_value)


def block_scale(stream_key, shape, shards, smallest, top_value):
    level = 1.0
    for position, parts in shards:
        steps = jax.random.uniform(jax.random.fold_in(jax.random.fold_in(stream_key, 6), position), (parts,), jnp.float32, smallest / len(shards), top_value / len(shards))
        level = level * jnp.repeat(jnp.exp(steps), shape[position] // parts).reshape((-1,) + (1,) * (len(shape) - 1 - position))
    return level


def gaussian(rng, dims, spread, most, cuts=(), dtype=jnp.bfloat16):
    array = spread * jax.random.normal(rng, dims, jnp.float32)
    if cuts:
        array = array * block_scale(rng, dims, cuts, -0.22, 0.18)
    return jnp.clip(array, -most, most).astype(dtype)


def setup_inputs(seed: int = 0) -> dict:
    seeds = jax.random.split(jax.random.key(seed), 6)
    return {
        "direct": gaussian(seeds[0], (P_SIZE, NT, N), 1.0, 6.0, ((0, 8), (2, 4))),
        "onsets": place_ends(jax.random.randint(seeds[1], (P_SIZE, N), NT // 8, NT), jax.random.fold_in(seeds[1], 1), NT // 8, NT - 1).astype(jnp.int32),
        "left_bases": gaussian(seeds[2], (F, NTL, NTL, 2, K, NB), (N // NB * K) ** -0.5, 0.4375, ((0, 8), (1, 4))),
        "right_bases": gaussian(seeds[3], (F, NTL, NTL, 2, K, NB), (2 * NB) ** -0.5, 0.25, ((0, 8), (1, 4))),
        "tile_ranks": place_ends(jax.random.randint(seeds[4], (F, NTL, NTL), 1, K + 1), jax.random.fold_in(seeds[4], 1), 1, K).astype(jnp.int32),
    }


HIGHEST = lax.Precision.HIGHEST

def band_tables(freq_total, sample_total):
    bins = lax.broadcasted_iota(jnp.int32, (freq_total, sample_total), 0) + 1
    moments = lax.broadcasted_iota(jnp.int32, (freq_total, sample_total), 1)
    phases = 2.0 * math.pi / sample_total * (bins * moments % sample_total).astype(jnp.float32)
    scaling = 1.0 / math.sqrt(sample_total)
    cosine = jnp.cos(phases) * scaling
    sine = jnp.sin(phases) * scaling
    return (jnp.stack([cosine, -sine]), jnp.stack([2.0 * cosine, -2.0 * sine]))

def rounded(values):
    return lax.optimization_barrier(values.astype(jnp.bfloat16)).astype(jnp.float32)

def contract(spec, left_part, right_part):
    return jnp.einsum(spec, left_part.astype(jnp.float32), right_part.astype(jnp.float32), precision=HIGHEST)

def conj_apply(spec, basis_real, basis_imag, vector_real, vector_imag):
    real_part = contract(spec, basis_real, vector_real) + contract(spec, basis_imag, vector_imag)
    imag_part = contract(spec, basis_real, vector_imag) - contract(spec, basis_imag, vector_real)
    return (real_part, imag_part)

def plain_apply(spec, basis_real, basis_imag, vector_real, vector_imag):
    real_part = contract(spec, basis_real, vector_real) - contract(spec, basis_imag, vector_imag)
    imag_part = contract(spec, basis_real, vector_imag) + contract(spec, basis_imag, vector_real)
    return (real_part, imag_part)

def reference(direct, onsets, left_bases, right_bases, tile_ranks):
    forward_exact, inverse_exact = band_tables(F, NT)
    forward_table = rounded(forward_exact)
    inverse_table = rounded(inverse_exact)
    point_total = direct.shape[0]
    tile_count = N // NB
    tile_group = tile_count // N_PTS
    moments = lax.broadcasted_iota(jnp.int32, direct.shape, 1)
    window = (moments < onsets[:, None, :]).astype(jnp.float32)
    rank_index = lax.broadcasted_iota(jnp.int32, tile_ranks.shape + (K,), 3)
    rank_mask = (rank_index < tile_ranks[..., None]).astype(jnp.float32)[..., None]

    def to_band(history):
        samples = rounded(history)
        spectrum = jnp.einsum('cft,ptn->cfpn', forward_table, samples, precision=HIGHEST)
        spectrum = spectrum.reshape(2, F, point_total, tile_count, NB).astype(jnp.bfloat16)
        return jnp.moveaxis(spectrum, 1, 0)

    def to_time(spectrum):
        flat = jnp.moveaxis(spectrum, 0, 1).reshape(2, F, point_total, N).astype(jnp.float32)
        return jnp.einsum('cft,cfpn->ptn', inverse_table, flat, precision=HIGHEST) * window

    def forward_one(operands):
        spectrum, left_part, right_part, mask_part = operands
        real_part, imag_part = conj_apply('ijkb,pjb->ijkp', right_part[:, :, 0], right_part[:, :, 1], spectrum[0], spectrum[1])
        terms = (jnp.stack([real_part, imag_part]) * mask_part).astype(jnp.bfloat16)
        real_part, imag_part = plain_apply('ijkb,ijkp->pib', left_part[:, :, 0], left_part[:, :, 1], terms[0], terms[1])
        return jnp.stack([real_part, imag_part]).astype(jnp.bfloat16)

    def adjoint_one(operands):
        spectrum, left_part, right_part, mask_part = operands
        real_part, imag_part = conj_apply('ijkb,pib->ijkp', left_part[:, :, 0], left_part[:, :, 1], spectrum[0], spectrum[1])
        terms = (jnp.stack([real_part, imag_part]) * mask_part).astype(jnp.bfloat16)
        terms = terms.reshape(2, N_PTS, tile_group, tile_count, K, point_total)
        grouped = right_part.reshape(N_PTS, tile_group, tile_count, 2, K, NB)
        real_part, imag_part = plain_apply('gijkb,gijkp->gpjb', grouped[:, :, :, 0], grouped[:, :, :, 1], terms[0], terms[1])
        partial_value = jnp.stack([real_part, imag_part], axis=1).astype(jnp.bfloat16)
        partial_value = lax.optimization_barrier(partial_value).astype(jnp.float32)
        return lax.optimization_barrier(jnp.sum(partial_value, axis=0)).astype(jnp.bfloat16)
    history = direct.astype(jnp.float32)
    plus_field = history
    minus_field = jnp.zeros_like(history)
    for iteration in range(ITERS):
        spectra = lax.map(forward_one, (to_band(history), left_bases, right_bases, rank_mask))
        reflected = to_time(spectra)
        minus_field = minus_field + reflected
        spectra = lax.map(adjoint_one, (to_band(reflected), left_bases, right_bases, rank_mask))
        history = to_time(spectra)
        plus_field = plus_field + history
    return (plus_field, minus_field)
```

```python
import functools
import math

import jax
import jax.numpy as jnp
from jax import lax
from jax.experimental import pallas as pl
from jax.experimental.pallas import tpu as pltpu
from jax.sharding import PartitionSpec as P

NB = 256
K = 8
F = 128
ITERS = 3
NT = 512
CORES = 2
MESH = pl.DeviceIdType.MESH
f32 = jnp.float32
bf16 = jnp.bfloat16


def band_tables(freq_total, sample_total):
    bins = lax.broadcasted_iota(jnp.int32, (freq_total, sample_total), 0) + 1
    moments = lax.broadcasted_iota(jnp.int32, (freq_total, sample_total), 1)
    phases = 2.0 * math.pi / sample_total * (bins * moments % sample_total).astype(f32)
    scaling = 1.0 / math.sqrt(sample_total)
    cosine = jnp.cos(phases) * scaling
    sine = jnp.sin(phases) * scaling
    return (jnp.stack([cosine, -sine], 1), jnp.stack([2.0 * cosine, -2.0 * sine], 1))


def dot_nt(a, b):
    return lax.dot_general(a, b, (((1,), (1,)), ((), ())), preferred_element_type=f32)


def dot_nn(a, b):
    return lax.dot_general(a, b, (((1,), (0,)), ((), ())), preferred_element_type=f32)


def block_mask(group, lines):
    shape = (group * lines, group * 2 * K)
    row = lax.broadcasted_iota(jnp.int32, shape, 0) // lines
    column = lax.broadcasted_iota(jnp.int32, shape, 1) // (2 * K)
    return row == column


def coefficients(x, basis, mask):
    points, width = x.shape[0] // 2, basis.shape[0] * 2 * K
    product = dot_nt(x, basis.reshape(width, NB))
    lane = lax.broadcasted_iota(jnp.int32, (points, width), 1)
    first = (lane // K) % 2 == 0
    real, imag = product[:points], product[points:]

    def other(value):
        return jnp.where(first, pltpu.roll(value, width - K, 1), -pltpu.roll(value, K, 1))

    both = jnp.concatenate([real + other(imag), imag - other(real)], axis=0)
    return (both * mask).astype(bf16)


def expand(terms, mask, group):
    return jnp.where(mask, jnp.concatenate([terms] * group, axis=0), jnp.zeros((), bf16))


class Places:
    def __init__(self, freq_size, pts_size):
        self.freq_size, self.pts_size = freq_size, pts_size
        self.columns = pts_size // CORES
        self.freq = lax.axis_index("freq")
        self.pts = lax.axis_index("pts")
        self.core = self.pts % CORES
        self.column = self.pts // CORES

    def freq_peer(self, step):
        return lax.rem(self.freq + step, self.freq_size)

    def freq_source(self, step):
        return lax.rem(self.freq + self.freq_size - step, self.freq_size)

    def sibling(self):
        return self.column * CORES + 1 - self.core

    def column_peer(self, step):
        return lax.rem(self.column + step, self.columns)

    def greet(self):
        barrier = pltpu.get_barrier_semaphore()
        for step in range(1, self.freq_size):
            pl.semaphore_signal(barrier, 1, device_id={"freq": self.freq_peer(step)}, device_id_type=MESH)
        pl.semaphore_signal(barrier, 1, device_id={"pts": self.sibling()}, device_id_type=MESH)
        for step in range(1, self.columns):
            peer = self.column_peer(step) * CORES + self.core
            pl.semaphore_signal(barrier, 1, device_id={"pts": peer}, device_id_type=MESH)
        pl.semaphore_wait(barrier, self.freq_size - 1 + 1 + self.columns - 1)


def remote(src, dst, send, recv, **device):
    return pltpu.make_async_remote_copy(
        src_ref=src, dst_ref=dst, send_sem=send, recv_sem=recv, device_id=device, device_id_type=MESH
    )


def load_bases(left_hbm, right_hbm, left, right, sems):
    copies = []
    for f in range(left.shape[0]):
        copies.append(pltpu.make_async_copy(right_hbm.at[f], right.at[f], sems.at[0, f]))
        copies.append(pltpu.make_async_copy(left_hbm.at[f], left.at[f], sems.at[1, f]))
    return copies


def rows_of(index, rows):
    return pl.ds(pl.multiple_of(index * rows, rows), rows)


def tile_of(index):
    return pl.ds(pl.multiple_of(index * NB, NB), NB)


def forward_kernel(
    sizes, spectrum, left_hbm, right_hbm, mask, order, back, result,
    left, right, got, total, outgoing, basis_sem,
    to_send, to_recv, home_send, home_recv, sib_send, sib_recv, col_send, col_recv,
    relay_send, relay_recv, ret_send, ret_recv, ret_home,
):
    freq_size, pts_size, rows, lines = sizes
    at = Places(freq_size, pts_size)
    freq_here, tiles = left.shape[0], left.shape[1]
    loads = load_bases(left_hbm, right_hbm, left, right, basis_sem)
    for copy in loads:
        copy.start()
    at.greet()

    def to_copy(j, step):
        peer = at.freq_peer(step)
        return remote(
            spectrum.at[rows_of(peer, rows), tile_of(j)],
            got.at[at.pts, j, rows_of(at.freq, rows), :],
            to_send.at[j, step], to_recv.at[j, step], freq=peer,
        )

    def home_copy(j):
        return pltpu.make_async_copy(
            spectrum.at[rows_of(at.freq, rows), tile_of(j)],
            got.at[at.pts, j, rows_of(at.freq, rows), :],
            home_send.at[j],
        )

    def sib_copy(j):
        return remote(
            got.at[at.pts, j], got.at[at.pts, j], sib_send.at[j], sib_recv.at[j], pts=at.sibling()
        )

    def col_copy(j, step):
        return remote(
            got.at[at.pts, j], got.at[at.pts, j], col_send.at[j, step], col_recv.at[j, step],
            pts=at.column_peer(step) * CORES + at.core,
        )

    def relay_copy(j, step):
        owner = lax.rem(at.column + at.columns - step, at.columns) * CORES + at.core
        return remote(
            got.at[owner, j], got.at[owner, j], relay_send.at[j, step], relay_recv.at[j, step],
            pts=at.sibling(),
        )

    def send(j, carry):
        for step in range(1, freq_size):
            to_copy(j, step).start()
        home_copy(j).start()
        return carry

    lax.fori_loop(0, tiles, send, 0)
    total[...] = jnp.zeros_like(total)
    spread = block_mask(tiles, lines)
    for copy in loads:
        copy.wait()

    def compute(owner, j):
        column = owner * tiles + j
        ordered = dot_nn(order[...], got[owner, j]).astype(bf16)
        terms = [
            coefficients(ordered[f * lines : (f + 1) * lines], right[f, :, column], mask[column, f : f + 1])
            for f in range(freq_here)
        ]
        for f in range(freq_here):
            total[f] += dot_nn(
                expand(terms[f], spread, tiles), left[f, :, column].reshape(tiles * 2 * K, NB)
            )

    def advance(j, carry):
        @pl.when(j < tiles)
        def _():
            for step in range(1, freq_size):
                to_copy(j, step).wait_recv()
            home_copy(j).wait()
            for step in range(1, at.columns):
                col_copy(j, step).start()
            sib_copy(j).start()

        @pl.when(j >= 1)
        def _():
            for step in range(1, at.columns):
                col_copy(j - 1, step).wait_recv()
                relay_copy(j - 1, step).start()

        @pl.when(j < tiles)
        def _():
            compute(at.pts, j)
            sib_copy(j).wait_recv()
            compute(at.sibling(), j)

        @pl.when(j >= 1)
        def _():
            for step in range(1, at.columns):
                source = lax.rem(at.column + at.columns - step, at.columns)
                compute(source * CORES + at.core, j - 1)
                relay_copy(j - 1, step).wait_recv()
                compute(source * CORES + 1 - at.core, j - 1)

        return carry

    lax.fori_loop(0, tiles + 1, advance, 0)
    finish = returning(at, rows, outgoing, result, ret_send, ret_recv, ret_home)
    for j in range(tiles):
        value = total[:, j * lines : (j + 1) * lines, :].reshape(freq_here * lines, NB)
        outgoing[j] = dot_nn(back[...], value.astype(bf16)).astype(bf16)
        finish.start(j)

    def drain(j, carry):
        for step in range(1, freq_size):
            to_copy(j, step).wait_send()
        sib_copy(j).wait_send()
        for step in range(1, at.columns):
            col_copy(j, step).wait_send()
            relay_copy(j, step).wait_send()
        finish.wait(j)
        return carry

    lax.fori_loop(0, tiles, drain, 0)


class returning:
    def __init__(self, at, rows, outgoing, result, send, recv, home):
        self.at, self.rows = at, rows
        self.outgoing, self.result = outgoing, result
        self.send, self.recv, self.home = send, recv, home

    def copy(self, j, step):
        peer = self.at.freq_peer(step)
        return remote(
            self.outgoing.at[j, rows_of(peer, self.rows), :],
            self.result.at[rows_of(self.at.freq, self.rows), tile_of(j)],
            self.send.at[j, step], self.recv.at[j, step], freq=peer,
        )

    def own(self, j):
        return pltpu.make_async_copy(
            self.outgoing.at[j, rows_of(self.at.freq, self.rows), :],
            self.result.at[rows_of(self.at.freq, self.rows), tile_of(j)],
            self.home.at[j],
        )

    def start(self, j):
        for step in range(1, self.at.freq_size):
            self.copy(j, step).start()
        self.own(j).start()

    def wait(self, j):
        for step in range(1, self.at.freq_size):
            self.copy(j, step).wait()
        self.own(j).wait()


def adjoint_kernel(
    sizes, spectrum, left_hbm, right_hbm, mask, order, back, result,
    left, right, got, total, outgoing, pair_out, pair_in, col_out, col_in, basis_sem,
    to_send, to_recv, home_send, pair_send, pair_recv, col_send, col_recv,
    ret_send, ret_recv, ret_home,
):
    freq_size, pts_size, rows, lines = sizes
    at = Places(freq_size, pts_size)
    freq_here, tiles = left.shape[0], left.shape[1]
    loads = load_bases(left_hbm, right_hbm, left, right, basis_sem)
    for copy in loads:
        copy.start()
    at.greet()

    def to_copy(j, step):
        peer = at.freq_peer(step)
        return remote(
            spectrum.at[rows_of(peer, rows), tile_of(j)],
            got.at[j, rows_of(at.freq, rows), :],
            to_send.at[j, step], to_recv.at[j, step], freq=peer,
        )

    def home_copy(j):
        return pltpu.make_async_copy(
            spectrum.at[rows_of(at.freq, rows), tile_of(j)],
            got.at[j, rows_of(at.freq, rows), :],
            home_send.at[j],
        )

    def send(j, carry):
        for step in range(1, freq_size):
            to_copy(j, step).start()
        home_copy(j).start()
        return carry

    lax.fori_loop(0, tiles, send, 0)
    total[...] = jnp.zeros_like(total)
    spread = block_mask(tiles, lines)
    for copy in loads:
        copy.wait()

    def advance(j, carry):
        for step in range(1, freq_size):
            to_copy(j, step).wait_recv()
        home_copy(j).wait()
        ordered = dot_nn(order[...], got[j]).astype(bf16)

        def group(owner, carry):
            span = pl.ds(owner * tiles, tiles)
            terms = [
                coefficients(ordered[f * lines : (f + 1) * lines], left[f, j, span], mask[j, owner, f : f + 1])
                for f in range(freq_here)
            ]
            for f in range(freq_here):
                total[owner, f] += dot_nn(
                    expand(terms[f], spread, tiles), right[f, j, span].reshape(tiles * 2 * K, NB)
                )
            return carry

        lax.fori_loop(0, pts_size, group, 0)
        return carry

    lax.fori_loop(0, tiles, advance, 0)

    def part(owner, j):
        piece = total[owner, :, pl.ds(pl.multiple_of(j * lines, lines), lines), :]
        return piece.reshape(freq_here * lines, NB)

    def pair_copy(j, step):
        return remote(
            pair_out.at[step, j], pair_in.at[step, j], pair_send.at[step, j], pair_recv.at[step, j],
            pts=at.sibling(),
        )

    def col_copy(j, step):
        return remote(
            col_out.at[step, j], col_in.at[step, j], col_send.at[step, j], col_recv.at[step, j],
            pts=at.column_peer(step) * CORES + at.core,
        )

    finish = returning(at, rows, outgoing, result, ret_send, ret_recv, ret_home)
    for step in list(range(1, at.columns)) + [0]:

        def pair_start(j, carry, step=step):
            owner = at.column_peer(step) * CORES + 1 - at.core
            pair_out[step, j] = part(owner, j).astype(bf16)
            pair_copy(j, step).start()
            return carry

        lax.fori_loop(0, tiles, pair_start, 0)
    for step in range(1, at.columns):

        def col_start(j, carry, step=step):
            pair_copy(j, step).wait_recv()
            owner = at.column_peer(step) * CORES + at.core
            col_out[step, j] = (part(owner, j) + pair_in[step, j].astype(f32)).astype(bf16)
            col_copy(j, step).start()
            return carry

        lax.fori_loop(0, tiles, col_start, 0)

    def close(j, carry):
        pair_copy(j, 0).wait_recv()
        value = part(at.pts, j) + pair_in[0, j].astype(f32)
        for step in range(1, at.columns):
            col_copy(j, step).wait_recv()
            value = value + col_in[step, j].astype(f32)
        outgoing[j] = dot_nn(back[...], value.astype(bf16)).astype(bf16)
        finish.start(j)
        return carry

    lax.fori_loop(0, tiles, close, 0)

    def drain(j, carry):
        for step in range(1, freq_size):
            to_copy(j, step).wait_send()
        for step in range(at.columns):
            pair_copy(j, step).wait_send()
        for step in range(1, at.columns):
            col_copy(j, step).wait_send()
        finish.wait(j)
        return carry

    lax.fori_loop(0, tiles, drain, 0)


def exchange_call(kind, sizes, spectrum, left, right, mask, order, back):
    freq_size, pts_size, rows, lines = sizes
    freq_here, tiles, tile_count = left.shape[:3]
    block = freq_size * rows
    columns = pts_size // CORES
    dma = pltpu.SemaphoreType.DMA
    bases = [pltpu.VMEM(left.shape, bf16), pltpu.VMEM(right.shape, bf16)]
    outgoing = pltpu.VMEM((tiles, block, NB), bf16)
    to_sems = [dma((tiles, freq_size)), dma((tiles, freq_size)), dma((tiles,))]
    ret_sems = [dma((tiles, freq_size)), dma((tiles, freq_size)), dma((tiles,))]
    if kind == "forward":
        kernel = forward_kernel
        scratch = bases + [
            pltpu.VMEM((pts_size, tiles, block, NB), bf16),
            pltpu.VMEM((freq_here, tiles * lines, NB), f32),
            outgoing,
            dma((2, freq_here)),
        ] + to_sems[:2] + [dma((tiles,)), dma((tiles,))] + [dma((tiles,)), dma((tiles,))] + [
            dma((tiles, columns)) for _ in range(4)
        ] + ret_sems
    else:
        kernel = adjoint_kernel
        pairs = [pltpu.VMEM((columns, tiles, block, NB), bf16) for _ in range(4)]
        scratch = bases + [
            pltpu.VMEM((tiles, block, NB), bf16),
            pltpu.VMEM((pts_size, freq_here, tiles * lines, NB), f32),
            outgoing,
        ] + pairs + [dma((2, freq_here))] + to_sems + [dma((columns, tiles)) for _ in range(4)] + ret_sems
    vmem = pl.BlockSpec(memory_space=pltpu.VMEM)
    hbm = pl.BlockSpec(memory_space=pl.ANY)
    return pl.pallas_call(
        functools.partial(kernel, sizes),
        out_shape=jax.ShapeDtypeStruct(spectrum.shape, bf16),
        name=kind,
        in_specs=[vmem, hbm, hbm, vmem, vmem, vmem],
        out_specs=vmem,
        scratch_shapes=scratch,
        compiler_params=pltpu.CompilerParams(
            collective_id=1 if kind == "forward" else 2,
            has_side_effects=True,
            vmem_limit_bytes=60 * 2**20,
        ),
    )(spectrum, left, right, mask, order, back)


def body(freq_size, pts_size, direct, onsets, left_bases, right_bases, tile_ranks):
    forward_exact, inverse_exact = band_tables(F, NT)
    forward_table = forward_exact.astype(bf16).reshape(2 * F, NT)
    inverse_table = inverse_exact.astype(bf16).reshape(2 * F, NT)
    point_here, _, cells_here = direct.shape
    freq_here, tiles, tile_count = left_bases.shape[:3]
    points = point_here * freq_size
    lines = 2 * points
    rows = point_here * freq_here * 2
    block = freq_size * rows
    sizes = (freq_size, pts_size, rows, lines)
    moments = lax.broadcasted_iota(jnp.int32, direct.shape, 1)
    window = moments < onsets[:, None, :]
    rank_index = lax.broadcasted_iota(jnp.int32, tile_ranks.shape + (2, K), 4)
    rank_mask = (rank_index < tile_ranks[..., None, None]).astype(f32)
    forward_mask = rank_mask.transpose(2, 0, 1, 3, 4).reshape(tile_count, freq_here, tiles * 2 * K)
    adjoint_mask = rank_mask.transpose(1, 2, 0, 3, 4).reshape(tiles, pts_size, tiles, freq_here, 2 * K)
    adjoint_mask = adjoint_mask.transpose(0, 1, 3, 2, 4).reshape(tiles, pts_size, freq_here, tiles * 2 * K)
    left = left_bases.reshape(freq_here, tiles, tile_count, 2 * K, NB)
    right = right_bases.reshape(freq_here, tiles, tile_count, 2 * K, NB)
    new = lax.broadcasted_iota(jnp.int32, (block, block), 0)
    old = lax.broadcasted_iota(jnp.int32, (block, block), 1)
    order = (new == old % (2 * freq_here) * points + old // (2 * freq_here)).astype(bf16)
    back = order.T

    def to_band(history):
        spectrum = jnp.einsum(
            "rt,ptn->prn", forward_table, history.astype(bf16), preferred_element_type=f32
        ).astype(bf16)
        spectrum = spectrum.reshape(point_here, freq_size, 2 * freq_here, cells_here)
        return spectrum.transpose(1, 0, 2, 3).reshape(block, cells_here)

    def to_time(result):
        result = result.reshape(freq_size, point_here, 2 * freq_here, cells_here).transpose(1, 0, 2, 3)
        result = result.reshape(point_here, 2 * F, cells_here)
        field = jnp.einsum("rt,prn->ptn", inverse_table, result, preferred_element_type=f32)
        return jnp.where(window, field, 0.0)

    history = direct.astype(f32)
    plus_field = history
    minus_field = jnp.zeros_like(history)
    for iteration in range(ITERS):
        reflected = to_time(
            exchange_call("forward", sizes, to_band(history), left, right, forward_mask, order, back)
        )
        minus_field = minus_field + reflected
        history = to_time(
            exchange_call("adjoint", sizes, to_band(reflected), left, right, adjoint_mask, order, back)
        )
        plus_field = plus_field + history
    return (plus_field, minus_field)


def solution(mesh):
    return jax.shard_map(
        functools.partial(body, mesh.shape["freq"], mesh.shape["pts"]),
        mesh=mesh,
        in_specs=(
            P("freq", None, "pts"),
            P("freq", "pts"),
            P("freq", "pts", None, None, None, None),
            P("freq", "pts", None, None, None, None),
            P("freq", "pts", None),
        ),
        out_specs=(P("freq", None, "pts"), P("freq", None, "pts")),
        check_vma=False,
    )
```

```python
import functools
import math

import jax
import jax.numpy as jnp
from jax import lax
from jax.experimental import pallas as pl
from jax.experimental.pallas import tpu as pltpu
from jax.sharding import PartitionSpec as P

NB = 256
K = 8
F = 128
ITERS = 3
NT = 512
CORES = 2
MESH = pl.DeviceIdType.MESH
f32 = jnp.float32
bf16 = jnp.bfloat16


def band_tables(freq_total, sample_total):
    bins = lax.broadcasted_iota(jnp.int32, (freq_total, sample_total), 0) + 1
    moments = lax.broadcasted_iota(jnp.int32, (freq_total, sample_total), 1)
    phases = 2.0 * math.pi / sample_total * (bins * moments % sample_total).astype(f32)
    scaling = 1.0 / math.sqrt(sample_total)
    cosine = jnp.cos(phases) * scaling
    sine = jnp.sin(phases) * scaling
    return (jnp.stack([cosine, -sine], 1), jnp.stack([2.0 * cosine, -2.0 * sine], 1))


def dot_nt(a, b):
    return lax.dot_general(a, b, (((1,), (1,)), ((), ())), preferred_element_type=f32)


def dot_nn(a, b):
    return lax.dot_general(a, b, (((1,), (0,)), ((), ())), preferred_element_type=f32)


def block_mask(group, lines, count):
    shape = (group * lines, count * group * 2 * K)
    row = lax.broadcasted_iota(jnp.int32, shape, 0) // lines
    column = lax.broadcasted_iota(jnp.int32, shape, 1) // (2 * K) % group
    return row == column


def coefficients(x, basis, mask):
    points, width = x.shape[0] // 2, basis.shape[0] * 2 * K
    product = dot_nt(x, basis.reshape(width, NB))
    lane = lax.broadcasted_iota(jnp.int32, (points, width), 1)
    first = (lane // K) % 2 == 0
    real, imag = product[:points], product[points:]

    def other(value):
        return jnp.where(first, pltpu.roll(value, width - K, 1), -pltpu.roll(value, K, 1))

    both = jnp.concatenate([real + other(imag), imag - other(real)], axis=0)
    return (both * mask).astype(bf16)


def rank_terms(pieces):
    return jnp.concatenate([coefficients(x, basis, mask) for x, basis, mask in pieces], axis=1)


def add_up(terms, spread, bases):
    group = bases[0].shape[0]
    weights = [basis.reshape(group * 2 * K, NB) for basis in bases]
    return dot_nn(expand(terms, spread, group), jnp.concatenate(weights, axis=0))


def expand(terms, mask, group):
    return jnp.where(mask, jnp.concatenate([terms] * group, axis=0), jnp.zeros((), bf16))


class Places:
    def __init__(self, freq_size, pts_size):
        self.freq_size, self.pts_size = freq_size, pts_size
        self.columns = pts_size // CORES
        self.freq = lax.axis_index("freq")
        self.pts = lax.axis_index("pts")
        self.core = self.pts % CORES
        self.column = self.pts // CORES

    def freq_peer(self, step):
        return lax.rem(self.freq + step, self.freq_size)

    def sibling(self):
        return self.column * CORES + 1 - self.core

    def column_peer(self, step):
        return lax.rem(self.column + step, self.columns)

    def column_source(self, step):
        return lax.rem(self.column + self.columns - step, self.columns)

    def greet(self):
        barrier = pltpu.get_barrier_semaphore()
        for step in range(1, self.freq_size):
            pl.semaphore_signal(barrier, 1, device_id={"freq": self.freq_peer(step)}, device_id_type=MESH)
        pl.semaphore_signal(barrier, 1, device_id={"pts": self.sibling()}, device_id_type=MESH)
        for step in range(1, self.columns):
            peer = self.column_peer(step) * CORES + self.core
            pl.semaphore_signal(barrier, 1, device_id={"pts": peer}, device_id_type=MESH)
        pl.semaphore_wait(barrier, self.freq_size - 1 + 1 + self.columns - 1)


def remote(src, dst, send, recv, **device):
    return pltpu.make_async_remote_copy(
        src_ref=src, dst_ref=dst, send_sem=send, recv_sem=recv, device_id=device, device_id_type=MESH
    )


def rows_of(index, rows):
    return pl.ds(pl.multiple_of(index * rows, rows), rows)


def series_kernel(
    sizes, direct, onsets, left_hbm, right_hbm, forward_mask, adjoint_mask, order, back, forward_table,
    inverse_table, kept, left, right, start, spectrum, got, own, total, outgoing, pair_out, pair_in,
    col_out, col_in, basis_sem, start_sem, to_send, to_recv, home_sem, sib_send, sib_recv, ring_send,
    ring_recv, relay_send, relay_recv, pair_send, pair_recv, col_send, col_recv, ret_send, ret_recv, ret_home,
):
    freq_size, pts_size, rows, lines = sizes
    at = Places(freq_size, pts_size)
    freq_here, tiles = left.shape[0], left.shape[1]
    spreads = {count: block_mask(tiles, lines, count) for count in (1, 2)}
    moments = lax.broadcasted_iota(jnp.int32, (NT, NB), 0)

    def start_copy(j):
        return pltpu.make_async_copy(
            direct.at[:, pl.ds(pl.multiple_of(j * NB, NB), NB)], start.at[j], start_sem.at[j]
        )

    def basis_copies(f):
        return [
            pltpu.make_async_copy(right_hbm.at[f], right.at[f], basis_sem.at[0, f]),
            pltpu.make_async_copy(left_hbm.at[f], left.at[f], basis_sem.at[1, f]),
        ]

    def to_copy(j, step, adjoint):
        peer = at.freq_peer(step)
        target = own.at[j] if adjoint else got.at[at.pts, j]
        return remote(
            spectrum.at[j, rows_of(peer, rows), :], target.at[rows_of(at.freq, rows), :],
            to_send.at[j, step], to_recv.at[j, step], freq=peer,
        )

    def home_copy(j, adjoint):
        target = own.at[j] if adjoint else got.at[at.pts, j]
        return pltpu.make_async_copy(
            spectrum.at[j, rows_of(at.freq, rows), :], target.at[rows_of(at.freq, rows), :], home_sem.at[j]
        )

    def sib_copy(j):
        return remote(
            got.at[at.pts, j], got.at[at.pts, j], sib_send.at[j], sib_recv.at[j], pts=at.sibling()
        )

    def ring_copy(j, step):
        return remote(
            got.at[at.pts, j], got.at[at.pts, j], ring_send.at[j, step], ring_recv.at[j, step],
            pts=at.column_peer(step) * CORES + at.core,
        )

    def relay_copy(j, step):
        owner = at.column_source(step) * CORES + at.core
        return remote(
            got.at[owner, j], got.at[owner, j], relay_send.at[j, step], relay_recv.at[j, step],
            pts=at.sibling(),
        )

    def pair_copy(j, step):
        return remote(
            pair_out.at[step, j], pair_in.at[step, j], pair_send.at[step, j], pair_recv.at[step, j],
            pts=at.sibling(),
        )

    def col_copy(j, step):
        return remote(
            col_out.at[step - 1, j], col_in.at[step - 1, j], col_send.at[step - 1, j],
            col_recv.at[step - 1, j], pts=at.column_peer(step) * CORES + at.core,
        )

    def ret_copy(j, step, half):
        peer = at.freq_peer(step)
        return remote(
            outgoing.at[j, rows_of(peer, rows), :], kept.at[half, j, rows_of(at.freq, rows), :],
            ret_send.at[j, step], ret_recv.at[j, step], freq=peer,
        )

    def ret_own(j, half):
        return pltpu.make_async_copy(
            outgoing.at[j, rows_of(at.freq, rows), :], kept.at[half, j, rows_of(at.freq, rows), :],
            ret_home.at[j],
        )

    def each(count, work):
        def step(j, carry):
            work(j)
            return carry

        lax.fori_loop(0, count, step, 0)

    def send_band(j, history, adjoint):
        spectrum[j] = dot_nn(forward_table[...], history).astype(bf16)
        for step in range(1, freq_size):
            to_copy(j, step, adjoint).start()
        home_copy(j, adjoint).start()

    def arrive(j, adjoint):
        for step in range(1, freq_size):
            to_copy(j, step, adjoint).wait_recv()
        home_copy(j, adjoint).wait()

    def send_back(j, value, half):
        outgoing[j] = dot_nn(back[...], value.astype(bf16)).astype(bf16)
        for step in range(1, freq_size):
            ret_copy(j, step, half).start()
        ret_own(j, half).start()

    def come_back(j, half):
        for step in range(1, freq_size):
            ret_copy(j, step, half).wait_recv()
        ret_own(j, half).wait()

    def turn(j, half, adjoint):
        field = dot_nn(inverse_table[...], kept[half, j])
        field = jnp.where(moments < onsets[j], field, 0.0)
        send_band(j, field.astype(bf16), adjoint)

    def part(owner, j):
        piece = total[owner, :, pl.ds(pl.multiple_of(j * lines, lines), lines), :]
        return piece.reshape(freq_here * lines, NB)

    def line_block(ordered, f):
        return ordered[f * lines : (f + 1) * lines]

    def forward_pair(owners, j):
        columns = [owner * tiles + j for owner in owners]
        ordered = [dot_nn(order[...], got[owner, j]).astype(bf16) for owner in owners]
        terms = [
            rank_terms(
                [
                    (line_block(x, f), right[f, :, c], forward_mask[c, f : f + 1])
                    for x, c in zip(ordered, columns)
                ]
            )
            for f in range(freq_here)
        ]
        for f in range(freq_here):
            total[0, f] += add_up(terms[f], spreads[2], [left[f, :, c] for c in columns])

    def forward_apply(half):
        total[0] = jnp.zeros(total.shape[1:], f32)

        def advance(j):
            @pl.when(j < tiles)
            def _():
                arrive(j, False)
                for step in range(1, at.columns):
                    ring_copy(j, step).start()
                sib_copy(j).start()

            @pl.when(j >= 1)
            def _():
                for step in range(1, at.columns):
                    ring_copy(j - 1, step).wait_recv()
                    relay_copy(j - 1, step).start()

            @pl.when(j < tiles)
            def _():
                sib_copy(j).wait_recv()
                forward_pair((at.pts, at.sibling()), j)

            @pl.when(j >= 1)
            def _():
                for step in range(1, at.columns):
                    source = at.column_source(step) * CORES
                    relay_copy(j - 1, step).wait_recv()
                    forward_pair((source + at.core, source + 1 - at.core), j - 1)

        each(tiles + 1, advance)

        def drain(j):
            for step in range(1, freq_size):
                to_copy(j, step, False).wait_send()
            sib_copy(j).wait_send()
            for step in range(1, at.columns):
                ring_copy(j, step).wait_send()
                relay_copy(j, step).wait_send()

        each(tiles, drain)
        each(tiles, lambda j: send_back(j, part(0, j), half))

    def adjoint_tiles(indices):
        for j in indices:
            arrive(j, True)
        ordered = [dot_nn(order[...], own[j]).astype(bf16) for j in indices]

        def group(owner):
            span = pl.ds(owner * tiles, tiles)
            terms = [
                rank_terms(
                    [
                        (line_block(x, f), left[f, j, span], adjoint_mask[j, owner, f : f + 1])
                        for x, j in zip(ordered, indices)
                    ]
                )
                for f in range(freq_here)
            ]
            spread = spreads[len(indices)]
            for f in range(freq_here):
                total[owner, f] += add_up(terms[f], spread, [right[f, j, span] for j in indices])

        each(pts_size, group)

    def adjoint_apply(half):
        total[...] = jnp.zeros_like(total)
        each(tiles // 2, lambda i: adjoint_tiles((2 * i, 2 * i + 1)))
        if tiles % 2:
            adjoint_tiles((tiles - 1,))
        for step in list(range(1, at.columns)) + [0]:

            def pair_start(j, step=step):
                owner = at.column_peer(step) * CORES + 1 - at.core
                pair_out[step, j] = part(owner, j).astype(bf16)
                pair_copy(j, step).start()

            each(tiles, pair_start)
        for step in range(1, at.columns):

            def col_start(j, step=step):
                pair_copy(j, step).wait_recv()
                owner = at.column_peer(step) * CORES + at.core
                col_out[step - 1, j] = (part(owner, j) + pair_in[step, j].astype(f32)).astype(bf16)
                col_copy(j, step).start()

            each(tiles, col_start)

        def close(j):
            pair_copy(j, 0).wait_recv()
            value = part(at.pts, j) + pair_in[0, j].astype(f32)
            for step in range(1, at.columns):
                col_copy(j, step).wait_recv()
                value = value + col_in[step - 1, j].astype(f32)
            send_back(j, value, half)

        each(tiles, close)

        def drain(j):
            for step in range(1, freq_size):
                to_copy(j, step, True).wait_send()
            for step in range(at.columns):
                pair_copy(j, step).wait_send()
            for step in range(1, at.columns):
                col_copy(j, step).wait_send()

        each(tiles, drain)

    def settle(half):
        def work(j):
            for step in range(1, freq_size):
                ret_copy(j, step, half).wait_send()

        each(tiles, work)

    each(tiles, lambda j: start_copy(j).start())
    for f in range(freq_here):
        for copy in basis_copies(f):
            copy.start()
    at.greet()

    def begin(j):
        start_copy(j).wait()
        send_band(j, start[j], False)

    each(tiles, begin)
    for f in range(freq_here):
        for copy in basis_copies(f):
            copy.wait()

    def iteration(i):
        forward_apply(2 * i)

        def go(j):
            come_back(j, 2 * i)
            turn(j, 2 * i, True)

        each(tiles, go)
        settle(2 * i)
        adjoint_apply(2 * i + 1)

        def again(j):
            come_back(j, 2 * i + 1)

            @pl.when(i < ITERS - 1)
            def _():
                turn(j, 2 * i + 1, False)

        each(tiles, again)
        settle(2 * i + 1)

    each(ITERS, iteration)


def series_call(sizes, direct, onsets, left, right, forward_mask, adjoint_mask, order, back, forward_table, inverse_table):
    freq_size, pts_size, rows, lines = sizes
    freq_here, tiles = left.shape[:2]
    block = freq_size * rows
    columns = pts_size // CORES
    dma = pltpu.SemaphoreType.DMA
    piece = (tiles, block, NB)
    scratch = [
        pltpu.VMEM(left.shape, bf16),
        pltpu.VMEM(right.shape, bf16),
        pltpu.VMEM((tiles, NT, NB), bf16),
        pltpu.VMEM(piece, bf16),
        pltpu.VMEM((pts_size,) + piece, bf16),
        pltpu.VMEM(piece, bf16),
        pltpu.VMEM((pts_size, freq_here, tiles * lines, NB), f32),
        pltpu.VMEM(piece, bf16),
        pltpu.VMEM((columns,) + piece, bf16),
        pltpu.VMEM((columns,) + piece, bf16),
        pltpu.VMEM((columns - 1,) + piece, bf16),
        pltpu.VMEM((columns - 1,) + piece, bf16),
        dma((2, freq_here)),
        dma((tiles,)),
        dma((tiles, freq_size)),
        dma((tiles, freq_size)),
        dma((tiles,)),
        dma((tiles,)),
        dma((tiles,)),
        dma((tiles, columns)),
        dma((tiles, columns)),
        dma((tiles, columns)),
        dma((tiles, columns)),
        dma((columns, tiles)),
        dma((columns, tiles)),
        dma((columns - 1, tiles)),
        dma((columns - 1, tiles)),
        dma((tiles, freq_size)),
        dma((tiles, freq_size)),
        dma((tiles,)),
    ]
    vmem = pl.BlockSpec(memory_space=pltpu.VMEM)
    hbm = pl.BlockSpec(memory_space=pl.ANY)
    return pl.pallas_call(
        functools.partial(series_kernel, sizes),
        out_shape=jax.ShapeDtypeStruct((2 * ITERS,) + piece, bf16),
        name="series",
        in_specs=[hbm, vmem, hbm, hbm] + [vmem] * 6,
        out_specs=vmem,
        scratch_shapes=scratch,
        compiler_params=pltpu.CompilerParams(
            collective_id=1, has_side_effects=True, vmem_limit_bytes=67043328
        ),
    )(direct, onsets, left, right, forward_mask, adjoint_mask, order, back, forward_table, inverse_table)


def fields_kernel(kept, direct, onsets, inverse_table, plus, minus):
    moments = lax.broadcasted_iota(jnp.int32, (NT, NB), 0)
    inside = moments < onsets[0]

    def total(first):
        value = dot_nn(inverse_table[...], kept[first, 0])
        for half in range(first + 2, 2 * ITERS, 2):
            value = value + dot_nn(inverse_table[...], kept[half, 0])
        return jnp.where(inside, value, 0.0)

    minus[...] = total(0)
    plus[...] = direct[...].astype(f32) + total(1)


def fields_call(kept, direct, onsets, inverse_table):
    tiles, block = kept.shape[1:3]
    field = pl.BlockSpec((NT, NB), lambda j: (0, j))
    return pl.pallas_call(
        fields_kernel,
        grid=(tiles,),
        out_shape=[jax.ShapeDtypeStruct(direct.shape, f32)] * 2,
        name="fields",
        in_specs=[
            pl.BlockSpec((2 * ITERS, 1, block, NB), lambda j: (0, j, 0, 0)),
            field,
            pl.BlockSpec((1, 1, NB), lambda j: (j, 0, 0)),
            pl.BlockSpec((NT, block), lambda j: (0, 0)),
        ],
        out_specs=[field, field],
    )(kept, direct, onsets, inverse_table)


def body(freq_size, pts_size, direct, onsets, left_bases, right_bases, tile_ranks):
    forward_exact, inverse_exact = band_tables(F, NT)
    forward_table = forward_exact.astype(bf16).reshape(2 * F, NT)
    inverse_table = inverse_exact.astype(bf16).reshape(2 * F, NT)
    point_here, _, cells_here = direct.shape
    freq_here, tiles, tile_count = left_bases.shape[:3]
    points = point_here * freq_size
    lines = 2 * points
    rows = point_here * freq_here * 2
    block = freq_size * rows
    sizes = (freq_size, pts_size, rows, lines)
    rank_index = lax.broadcasted_iota(jnp.int32, tile_ranks.shape + (2, K), 4)
    rank_mask = (rank_index < tile_ranks[..., None, None]).astype(f32)
    forward_mask = rank_mask.transpose(2, 0, 1, 3, 4).reshape(tile_count, freq_here, tiles * 2 * K)
    adjoint_mask = rank_mask.transpose(1, 2, 0, 3, 4).reshape(tiles, pts_size, tiles, freq_here, 2 * K)
    adjoint_mask = adjoint_mask.transpose(0, 1, 3, 2, 4).reshape(tiles, pts_size, freq_here, tiles * 2 * K)
    left = left_bases.reshape(freq_here, tiles, tile_count, 2 * K, NB)
    right = right_bases.reshape(freq_here, tiles, tile_count, 2 * K, NB)
    new = lax.broadcasted_iota(jnp.int32, (block, block), 0)
    old = lax.broadcasted_iota(jnp.int32, (block, block), 1)
    order = (new == old % (2 * freq_here) * points + old // (2 * freq_here)).astype(bf16)
    back = order.T

    assert point_here == 1
    onsets = onsets.reshape(tiles, 1, NB)
    inverse_table = inverse_table.T
    kept = series_call(
        sizes, direct[0], onsets, left, right, forward_mask, adjoint_mask, order, back, forward_table, inverse_table
    )
    plus_field, minus_field = fields_call(kept, direct[0], onsets, inverse_table)
    return (plus_field[None], minus_field[None])


def solution(mesh):
    return jax.shard_map(
        functools.partial(body, mesh.shape["freq"], mesh.shape["pts"]),
        mesh=mesh,
        in_specs=(
            P("freq", None, "pts"),
            P("freq", "pts"),
            P("freq", "pts", None, None, None, None),
            P("freq", "pts", None, None, None, None),
            P("freq", "pts", None),
        ),
        out_specs=(P("freq", None, "pts"), P("freq", None, "pts")),
        check_vma=False,
    )
```

```python
import functools
import math

import jax
import jax.numpy as jnp
import numpy as np
from jax import lax
from jax.experimental import pallas as pl
from jax.experimental.pallas import tpu as pltpu
from jax.sharding import PartitionSpec as P

NB = 256
K = 8
F = 128
ITERS = 3
NT = 512
CORES = 2
LAG = 2
RING_LAG = 3
TILE_LAG = 5
MESH = pl.DeviceIdType.MESH
f32 = jnp.float32
bf16 = jnp.bfloat16


def band_tables(freq_total, sample_total, freq_size, stages):
    bins = np.arange(1, freq_total + 1)[:, None]
    phases = 2.0 * math.pi / sample_total * (bins * np.arange(sample_total) % sample_total)
    parts = np.stack([np.cos(phases), -np.sin(phases)], 1) / math.sqrt(sample_total)
    parts = parts.reshape(freq_size, stages, -1, sample_total).transpose(1, 0, 2, 3).reshape(-1, sample_total)
    return parts.astype(np.float32).astype(bf16), (2.0 * parts).astype(np.float32).astype(bf16)


def dot_nt(a, b):
    return lax.dot_general(a, b, (((1,), (1,)), ((), ())), preferred_element_type=f32)


def dot_nn(a, b):
    return lax.dot_general(a, b, (((1,), (0,)), ((), ())), preferred_element_type=f32)


def block_mask(group, lines, count):
    shape = (group * lines, count * group * 2 * K)
    row = lax.broadcasted_iota(jnp.int32, shape, 0) // lines
    column = lax.broadcasted_iota(jnp.int32, shape, 1) // (2 * K) % group
    return row == column


def coefficients(x, basis, mask):
    points, width = x.shape[0] // 2, basis.shape[0] * 2 * K
    product = dot_nt(x, basis.reshape(width, NB))
    lane = lax.broadcasted_iota(jnp.int32, (points, width), 1)
    first = (lane // K) % 2 == 0
    real, imag = product[:points], product[points:]

    def other(value):
        return jnp.where(first, pltpu.roll(value, width - K, 1), -pltpu.roll(value, K, 1))

    both = jnp.concatenate([real + other(imag), imag - other(real)], axis=0)
    return (both * mask).astype(bf16)


def rank_terms(pieces):
    return jnp.concatenate([coefficients(x, basis, mask) for x, basis, mask in pieces], axis=1)


def add_up(terms, spread, bases):
    group = bases[0].shape[0]
    weights = [basis.reshape(group * 2 * K, NB) for basis in bases]
    return dot_nn(expand(terms, spread, group), jnp.concatenate(weights, axis=0))


def expand(terms, mask, group):
    return jnp.where(mask, jnp.concatenate([terms] * group, axis=0), jnp.zeros((), bf16))


class Places:
    def __init__(self, freq_size, pts_size):
        self.freq_size, self.pts_size = freq_size, pts_size
        self.columns = pts_size // CORES
        self.freq = lax.axis_index("freq")
        self.pts = lax.axis_index("pts")
        self.core = self.pts % CORES
        self.column = self.pts // CORES

    def freq_peer(self, step):
        return lax.rem(self.freq + step, self.freq_size)

    def sibling(self):
        return self.column * CORES + 1 - self.core

    def column_peer(self, step):
        return lax.rem(self.column + step, self.columns)

    def column_source(self, step):
        return lax.rem(self.column + self.columns - step, self.columns)

    def greet(self):
        barrier = pltpu.get_barrier_semaphore()
        for step in range(1, self.freq_size):
            pl.semaphore_signal(barrier, 1, device_id={"freq": self.freq_peer(step)}, device_id_type=MESH)
        pl.semaphore_signal(barrier, 1, device_id={"pts": self.sibling()}, device_id_type=MESH)
        for step in range(1, self.columns):
            peer = self.column_peer(step) * CORES + self.core
            pl.semaphore_signal(barrier, 1, device_id={"pts": peer}, device_id_type=MESH)
        pl.semaphore_wait(barrier, self.freq_size - 1 + 1 + self.columns - 1)


def remote(src, dst, send, recv, **device):
    return pltpu.make_async_remote_copy(
        src_ref=src, dst_ref=dst, send_sem=send, recv_sem=recv, device_id=device, device_id_type=MESH
    )


def rows_of(index, rows):
    return pl.ds(pl.multiple_of(index * rows, rows), rows)


def series_kernel(
    sizes, direct, onsets, left_hbm, right_hbm, forward_mask, adjoint_mask, order, back, forward_table,
    inverse_table, kept, left, right, start, spectrum, got, own, ahead, total, outgoing, pair_out, pair_in,
    col_out, col_in, basis_sem, start_sem, to_send, to_recv, home_sem, sib_send, sib_recv, ring_send,
    ring_recv, relay_send, relay_recv, pair_send, pair_recv, col_send, col_recv, ret_send, ret_recv, ret_home,
):
    freq_size, pts_size, stages, rows, lines = sizes
    at = Places(freq_size, pts_size)
    freq_here, tiles = left.shape[0], left.shape[1]
    inner = freq_here // stages
    block = freq_size * rows
    spreads = {count: block_mask(tiles, lines, count) for count in {1, 2, pts_size}}
    moments = lax.broadcasted_iota(jnp.int32, (NT, NB), 0)

    def start_copy(j):
        return pltpu.make_async_copy(
            direct.at[:, pl.ds(pl.multiple_of(j * NB, NB), NB)], start.at[j], start_sem.at[j]
        )

    def basis_copies(f):
        return [
            pltpu.make_async_copy(right_hbm.at[f], right.at[f], basis_sem.at[0, f]),
            pltpu.make_async_copy(left_hbm.at[f], left.at[f], basis_sem.at[1, f]),
        ]

    def to_copy(h, j, step, adjoint):
        peer = at.freq_peer(step)
        target = own.at[h, j] if adjoint else got.at[h, at.pts, j]
        return remote(
            spectrum.at[h, j, rows_of(peer, rows), :], target.at[rows_of(at.freq, rows), :],
            to_send.at[h, j, step], to_recv.at[h, j, step], freq=peer,
        )

    def home_copy(h, j, adjoint):
        target = own.at[h, j] if adjoint else got.at[h, at.pts, j]
        return pltpu.make_async_copy(
            spectrum.at[h, j, rows_of(at.freq, rows), :], target.at[rows_of(at.freq, rows), :], home_sem.at[h, j]
        )

    def sib_copy(h, j):
        mine = got.at[h, at.pts, j]
        return remote(mine, mine, sib_send.at[h, j], sib_recv.at[h, j], pts=at.sibling())

    def ring_copy(h, j, step):
        mine = got.at[h, at.pts, j]
        return remote(
            mine, mine, ring_send.at[h, j, step], ring_recv.at[h, j, step],
            pts=at.column_peer(step) * CORES + at.core,
        )

    def relay_copy(h, j, step):
        passed = got.at[h, at.column_source(step) * CORES + at.core, j]
        return remote(
            passed, passed, relay_send.at[h, j, step], relay_recv.at[h, j, step], pts=at.sibling()
        )

    def pair_copy(h, j, step):
        return remote(
            pair_out.at[h, step, j], pair_in.at[h, step, j], pair_send.at[h, step, j],
            pair_recv.at[h, step, j], pts=at.sibling(),
        )

    def col_copy(h, j, step):
        return remote(
            col_out.at[h, step - 1, j], col_in.at[h, step - 1, j], col_send.at[h, step - 1, j],
            col_recv.at[h, step - 1, j], pts=at.column_peer(step) * CORES + at.core,
        )

    def ret_copy(h, j, step, half):
        peer = at.freq_peer(step)
        return remote(
            outgoing.at[h, j, rows_of(peer, rows), :], kept.at[half, h, j, rows_of(at.freq, rows), :],
            ret_send.at[h, j, step], ret_recv.at[h, j, step], freq=peer,
        )

    def ret_own(h, j, half):
        return pltpu.make_async_copy(
            outgoing.at[h, j, rows_of(at.freq, rows), :], kept.at[half, h, j, rows_of(at.freq, rows), :],
            ret_home.at[h, j],
        )

    def each(count, work):
        def step(j, carry):
            work(j)
            return carry

        lax.fori_loop(0, count, step, 0)

    def send_stage(h, j, adjoint):
        for step in range(1, freq_size):
            to_copy(h, j, step, adjoint).start()
        home_copy(h, j, adjoint).start()

    def send_band(j, history, adjoint):
        bands = dot_nn(forward_table[...], history).astype(bf16)
        for h in range(stages):
            spectrum[h, j] = bands[h * block : (h + 1) * block]
        send_stage(0, j, adjoint)

    def send_rest(adjoint):
        for h in range(1, stages):
            each(tiles, lambda j, h=h: send_stage(h, j, adjoint))

    def arrive(h, j, adjoint):
        for step in range(1, freq_size):
            to_copy(h, j, step, adjoint).wait_recv()
        home_copy(h, j, adjoint).wait()

    def send_back(h, j, value, half):
        outgoing[h, j] = dot_nn(back[...], value.astype(bf16)).astype(bf16)
        for step in range(1, freq_size):
            ret_copy(h, j, step, half).start()
        ret_own(h, j, half).start()

    def come_back(j, half):
        for h in range(stages):
            for step in range(1, freq_size):
                ret_copy(h, j, step, half).wait_recv()
            ret_own(h, j, half).wait()

    def turn(j, half, adjoint):
        spectra = jnp.concatenate([kept[half, h, j] for h in range(stages)], axis=0)
        field = dot_nn(inverse_table[...], spectra)
        field = jnp.where(moments < onsets[j], field, 0.0)
        send_band(j, field.astype(bf16), adjoint)

    def piece_of(value):
        return value.reshape(inner * lines, NB)

    def lines_of(j):
        return pl.ds(pl.multiple_of(j * lines, lines), lines)

    def part(h, owner, j):
        return piece_of(total[owner, h * inner : (h + 1) * inner, lines_of(j), :])

    def line_block(ordered, f):
        return ordered[f * lines : (f + 1) * lines]

    def forward_tiles(h, owners, j):
        columns = [owner * tiles + j for owner in owners]
        ordered = [dot_nn(order[...], got[h, owner, j]).astype(bf16) for owner in owners]
        first = h * inner
        terms = [
            rank_terms(
                [
                    (line_block(x, f), right[first + f, :, c], forward_mask[c, h, f : f + 1])
                    for x, c in zip(ordered, columns)
                ]
            )
            for f in range(inner)
        ]
        for f in range(inner):
            ahead[first + f] += add_up(terms[f], spreads[len(owners)], [left[first + f, :, c] for c in columns])

    def forward_stages(half):
        count = stages * tiles

        def advance(t):
            @pl.when(t < count)
            def _():
                h, j = t // tiles, t % tiles
                arrive(h, j, False)
                for step in range(1, at.columns):
                    ring_copy(h, j, step).start()
                sib_copy(h, j).start()

            @pl.when((t >= RING_LAG) & (t < count + RING_LAG))
            def _():
                m = t - RING_LAG
                h, j = m // tiles, m % tiles
                for step in range(1, at.columns):
                    ring_copy(h, j, step).wait_recv()
                    relay_copy(h, j, step).start()

            @pl.when(t >= TILE_LAG)
            def _():
                m = t - TILE_LAG
                h, j = m // tiles, m % tiles
                sib_copy(h, j).wait_recv()
                owners = [at.pts, at.sibling()]
                for step in range(1, at.columns):
                    relay_copy(h, j, step).wait_recv()
                    source = at.column_source(step) * CORES
                    owners += [source + at.core, source + 1 - at.core]
                forward_tiles(h, owners, j)

            for h in range(stages):

                @pl.when(t == TILE_LAG + (h + 1) * tiles - 1)
                def _(h=h):
                    def back_now(j):
                        value = ahead[h * inner : (h + 1) * inner, lines_of(j), :]
                        send_back(h, j, piece_of(value), half)

                    each(tiles, back_now)

        each(count + TILE_LAG, advance)

    def adjoint_tiles(h, indices):
        for j in indices:
            arrive(h, j, True)
        ordered = [dot_nn(order[...], own[h, j]).astype(bf16) for j in indices]
        first = h * inner

        spread = spreads[len(indices)]

        def group(number):
            owners = [number * CORES + core for core in range(CORES)]
            spans = [pl.ds(owner * tiles, tiles) for owner in owners]
            terms = [
                rank_terms(
                    [
                        (
                            line_block(x, f),
                            left[first + f, j, span],
                            adjoint_mask[j, owner, first + f : first + f + 1],
                        )
                        for x, j in zip(ordered, indices)
                    ]
                )
                for owner, span in zip(owners, spans)
                for f in range(inner)
            ]
            for n, (owner, span) in enumerate(zip(owners, spans)):
                for f in range(inner):
                    bases = [right[first + f, j, span] for j in indices]
                    total[owner, first + f] += add_up(terms[n * inner + f], spread, bases)

        each(at.columns, group)

    def adjoint_stage(h, half):
        pairs = tiles // 2

        def two(n):
            adjoint_tiles(h, (2 * n, 2 * n + 1))
            if h:
                close(h - 1, 2 * n, half)
                close(h - 1, 2 * n + 1, half)

        each(pairs, two)
        if tiles % 2:
            adjoint_tiles(h, (tiles - 1,))
            if h:
                close(h - 1, tiles - 1, half)

    def reduce_start(h):
        for step in list(range(1, at.columns)) + [0]:

            def pair_start(j, step=step):
                owner = at.column_peer(step) * CORES + 1 - at.core
                pair_out[h, step, j] = part(h, owner, j).astype(bf16)
                pair_copy(h, j, step).start()

            each(tiles, pair_start)
        for step in range(1, at.columns):

            def col_start(j, step=step):
                pair_copy(h, j, step).wait_recv()
                owner = at.column_peer(step) * CORES + at.core
                value = part(h, owner, j) + pair_in[h, step, j].astype(f32)
                col_out[h, step - 1, j] = value.astype(bf16)
                col_copy(h, j, step).start()

            each(tiles, col_start)

    def close(h, j, half):
        pair_copy(h, j, 0).wait_recv()
        value = part(h, at.pts, j) + pair_in[h, 0, j].astype(f32)
        for step in range(1, at.columns):
            col_copy(h, j, step).wait_recv()
            value = value + col_in[h, step - 1, j].astype(f32)
        send_back(h, j, value, half)

    def to_drain(j, adjoint):
        for h in range(stages):
            for step in range(1, freq_size):
                to_copy(h, j, step, adjoint).wait_send()

    def reduce_drain(j):
        for h in range(stages):
            for step in range(at.columns):
                pair_copy(h, j, step).wait_send()
            for step in range(1, at.columns):
                col_copy(h, j, step).wait_send()

    def gather_drain(j):
        to_drain(j, False)
        for h in range(stages):
            sib_copy(h, j).wait_send()
            for step in range(1, at.columns):
                ring_copy(h, j, step).wait_send()
                relay_copy(h, j, step).wait_send()

    def ret_drain(j, half):
        for h in range(stages):
            for step in range(1, freq_size):
                ret_copy(h, j, step, half).wait_send()

    each(tiles, lambda j: start_copy(j).start())
    for f in range(freq_here):
        for copy in basis_copies(f):
            copy.start()
    at.greet()

    def begin(j):
        start_copy(j).wait()
        send_band(j, start[j], False)

    each(tiles, begin)
    send_rest(False)
    for f in range(freq_here):
        for copy in basis_copies(f):
            copy.wait()

    def iteration(i):
        half = 2 * i
        ahead[...] = jnp.zeros_like(ahead)
        forward_stages(half)
        each(tiles, gather_drain)
        total[...] = jnp.zeros_like(total)

        def go(j):
            come_back(j, half)
            turn(j, half, True)

        each(tiles, go)
        send_rest(True)
        each(tiles, lambda j: ret_drain(j, half))
        for h in range(stages):
            adjoint_stage(h, half + 1)
            reduce_start(h)
        each(tiles, lambda j: to_drain(j, True))

        def last(t):
            @pl.when(t < tiles)
            def _():
                close(stages - 1, t, half + 1)

            @pl.when(t >= LAG)
            def _():
                come_back(t - LAG, half + 1)

            @pl.when((t >= LAG) & (i < ITERS - 1))
            def _():
                turn(t - LAG, half + 1, False)

        each(tiles + LAG, last)

        @pl.when(i < ITERS - 1)
        def _():
            send_rest(False)

        each(tiles, lambda j: ret_drain(j, half + 1))
        each(tiles, reduce_drain)

    each(ITERS, iteration)


def series_call(sizes, direct, onsets, left, right, forward_mask, adjoint_mask, order, back, forward_table, inverse_table):
    freq_size, pts_size, stages, rows, lines = sizes
    freq_here, tiles = left.shape[:2]
    block = freq_size * rows
    columns = pts_size // CORES
    dma = pltpu.SemaphoreType.DMA
    piece = (tiles, block, NB)
    scratch = [
        pltpu.VMEM(left.shape, bf16),
        pltpu.VMEM(right.shape, bf16),
        pltpu.VMEM((tiles, NT, NB), bf16),
        pltpu.VMEM((stages,) + piece, bf16),
        pltpu.VMEM((stages, pts_size) + piece, bf16),
        pltpu.VMEM((stages,) + piece, bf16),
        pltpu.VMEM((freq_here, tiles * lines, NB), f32),
        pltpu.VMEM((pts_size, freq_here, tiles * lines, NB), f32),
        pltpu.VMEM((stages,) + piece, bf16),
        pltpu.VMEM((stages, columns) + piece, bf16),
        pltpu.VMEM((stages, columns) + piece, bf16),
        pltpu.VMEM((stages, columns - 1) + piece, bf16),
        pltpu.VMEM((stages, columns - 1) + piece, bf16),
        dma((2, freq_here)),
        dma((tiles,)),
        dma((stages, tiles, freq_size)),
        dma((stages, tiles, freq_size)),
        dma((stages, tiles)),
        dma((stages, tiles)),
        dma((stages, tiles)),
        dma((stages, tiles, columns)),
        dma((stages, tiles, columns)),
        dma((stages, tiles, columns)),
        dma((stages, tiles, columns)),
        dma((stages, columns, tiles)),
        dma((stages, columns, tiles)),
        dma((stages, columns - 1, tiles)),
        dma((stages, columns - 1, tiles)),
        dma((stages, tiles, freq_size)),
        dma((stages, tiles, freq_size)),
        dma((stages, tiles)),
    ]
    vmem = pl.BlockSpec(memory_space=pltpu.VMEM)
    hbm = pl.BlockSpec(memory_space=pl.ANY)
    return pl.pallas_call(
        functools.partial(series_kernel, sizes),
        out_shape=jax.ShapeDtypeStruct((2 * ITERS, stages) + piece, bf16),
        name="series",
        in_specs=[hbm, vmem, hbm, hbm] + [vmem] * 6,
        out_specs=vmem,
        scratch_shapes=scratch,
        compiler_params=pltpu.CompilerParams(
            collective_id=1, has_side_effects=True, vmem_limit_bytes=67043328
        ),
    )(direct, onsets, left, right, forward_mask, adjoint_mask, order, back, forward_table, inverse_table)


def fields_kernel(kept, direct, onsets, inverse_table, plus, minus):
    moments = lax.broadcasted_iota(jnp.int32, (NT, NB), 0)
    inside = moments < onsets[0]

    def total(first):
        spectra = jnp.concatenate(
            [kept[half, h, 0] for half in range(first, 2 * ITERS, 2) for h in range(kept.shape[1])], axis=0
        )
        value = dot_nn(inverse_table[...], spectra)
        return jnp.where(inside, value, 0.0)

    minus[...] = total(0)
    plus[...] = direct[...].astype(f32) + total(1)


def fields_call(kept, direct, onsets, inverse_table):
    stages, tiles, block = kept.shape[1:4]
    field = pl.BlockSpec((NT, NB), lambda j: (0, j))
    return pl.pallas_call(
        fields_kernel,
        grid=(tiles,),
        out_shape=[jax.ShapeDtypeStruct(direct.shape, f32)] * 2,
        name="fields",
        in_specs=[
            pl.BlockSpec((2 * ITERS, stages, 1, block, NB), lambda j: (0, 0, j, 0, 0)),
            field,
            pl.BlockSpec((1, 1, NB), lambda j: (j, 0, 0)),
            pl.BlockSpec((NT, ITERS * stages * block), lambda j: (0, 0)),
        ],
        out_specs=[field, field],
    )(kept, direct, onsets, inverse_table)


def body(freq_size, pts_size, direct, onsets, left_bases, right_bases, tile_ranks):
    point_here, _, cells_here = direct.shape
    assert point_here == 1
    freq_here, tiles, tile_count = left_bases.shape[:3]
    points = point_here * freq_size
    lines = 2 * points
    stages = 2 if freq_here % 16 == 0 else 1
    inner = freq_here // stages
    rows = inner * 2
    block = freq_size * rows
    sizes = (freq_size, pts_size, stages, rows, lines)
    forward_table, inverse_table = band_tables(F, NT, freq_size, stages)
    inverse_table = np.ascontiguousarray(inverse_table.T)
    rank_index = lax.broadcasted_iota(jnp.int32, tile_ranks.shape + (2, K), 4)
    rank_mask = (rank_index < tile_ranks[..., None, None]).astype(f32)
    forward_mask = rank_mask.transpose(2, 0, 1, 3, 4).reshape(tile_count, stages, inner, tiles * 2 * K)
    adjoint_mask = rank_mask.transpose(1, 2, 0, 3, 4).reshape(tiles, pts_size, tiles, freq_here, 2 * K)
    adjoint_mask = adjoint_mask.transpose(0, 1, 3, 2, 4).reshape(tiles, pts_size, freq_here, tiles * 2 * K)
    left = left_bases.reshape(freq_here, tiles, tile_count, 2 * K, NB)
    right = right_bases.reshape(freq_here, tiles, tile_count, 2 * K, NB)
    old = np.arange(block)
    order = np.zeros((block, block), np.float32)
    order[old % rows * points + old // rows, old] = 1.0
    order = order.astype(bf16)
    back = np.ascontiguousarray(order.T)
    onsets = onsets.reshape(tiles, 1, NB)
    kept = series_call(
        sizes, direct[0], onsets, left, right, forward_mask, adjoint_mask, order, back, forward_table, inverse_table
    )
    plus_field, minus_field = fields_call(kept, direct[0], onsets, np.concatenate([inverse_table] * ITERS, axis=1))
    return (plus_field[None], minus_field[None])


def solution(mesh):
    return jax.shard_map(
        functools.partial(body, mesh.shape["freq"], mesh.shape["pts"]),
        mesh=mesh,
        in_specs=(
            P("freq", None, "pts"),
            P("freq", "pts"),
            P("freq", "pts", None, None, None, None),
            P("freq", "pts", None, None, None, None),
            P("freq", "pts", None),
        ),
        out_specs=(P("freq", None, "pts"), P("freq", None, "pts")),
        check_vma=False,
    )
```

```python
import functools
import math

import jax
import jax.numpy as jnp
import numpy as np
from jax import lax
from jax.experimental import pallas as pl
from jax.experimental.pallas import tpu as pltpu
from jax.sharding import PartitionSpec as P

NB = 256
K = 8
F = 128
ITERS = 3
NT = 512
CORES = 2
LAG = 5
RING_LAG = 3
TILE_LAG = 5
MESH = pl.DeviceIdType.MESH
f32 = jnp.float32
bf16 = jnp.bfloat16


def band_tables(freq_total, sample_total, freq_size, stages):
    bins = np.arange(1, freq_total + 1)[:, None]
    phases = 2.0 * math.pi / sample_total * (bins * np.arange(sample_total) % sample_total)
    parts = np.stack([np.cos(phases), -np.sin(phases)], 1) / math.sqrt(sample_total)
    parts = parts.reshape(freq_size, stages, -1, sample_total).transpose(1, 0, 2, 3).reshape(-1, sample_total)
    return parts.astype(np.float32).astype(bf16), (2.0 * parts).astype(np.float32).astype(bf16)


def dot_nt(a, b):
    return lax.dot_general(a, b, (((1,), (1,)), ((), ())), preferred_element_type=f32)


def dot_nn(a, b):
    return lax.dot_general(a, b, (((1,), (0,)), ((), ())), preferred_element_type=f32)


def block_mask(group, lines, count):
    shape = (group * lines, count * group * 2 * K)
    row = lax.broadcasted_iota(jnp.int32, shape, 0) // lines
    column = lax.broadcasted_iota(jnp.int32, shape, 1) // (2 * K) % group
    return row == column


def coefficients(x, basis, mask):
    points, width = x.shape[0] // 2, basis.shape[0] * 2 * K
    product = dot_nt(x, basis.reshape(width, NB))
    lane = lax.broadcasted_iota(jnp.int32, (points, width), 1)
    first = (lane // K) % 2 == 0
    real, imag = product[:points], product[points:]

    def other(value):
        return jnp.where(first, pltpu.roll(value, width - K, 1), -pltpu.roll(value, K, 1))

    both = jnp.concatenate([real + other(imag), imag - other(real)], axis=0)
    return (both * mask).astype(bf16)


def rank_terms(pieces):
    return jnp.concatenate([coefficients(x, basis, mask) for x, basis, mask in pieces], axis=1)


def add_up(terms, spread, bases):
    group = bases[0].shape[0]
    weights = [basis.reshape(group * 2 * K, NB) for basis in bases]
    return dot_nn(expand(terms, spread, group), jnp.concatenate(weights, axis=0))


def expand(terms, mask, group):
    return jnp.where(mask, jnp.concatenate([terms] * group, axis=0), jnp.zeros((), bf16))


class Places:
    def __init__(self, freq_size, pts_size):
        self.freq_size, self.pts_size = freq_size, pts_size
        self.columns = pts_size // CORES
        self.freq = lax.axis_index("freq")
        self.pts = lax.axis_index("pts")
        self.core = self.pts % CORES
        self.column = self.pts // CORES

    def freq_peer(self, step):
        return lax.rem(self.freq + step, self.freq_size)

    def sibling(self):
        return self.column * CORES + 1 - self.core

    def column_peer(self, step):
        return lax.rem(self.column + step, self.columns)

    def column_source(self, step):
        return lax.rem(self.column + self.columns - step, self.columns)

    def greet(self):
        barrier = pltpu.get_barrier_semaphore()
        for step in range(1, self.freq_size):
            pl.semaphore_signal(barrier, 1, device_id={"freq": self.freq_peer(step)}, device_id_type=MESH)
        pl.semaphore_signal(barrier, 1, device_id={"pts": self.sibling()}, device_id_type=MESH)
        for step in range(1, self.columns):
            peer = self.column_peer(step) * CORES + self.core
            pl.semaphore_signal(barrier, 1, device_id={"pts": peer}, device_id_type=MESH)
        pl.semaphore_wait(barrier, self.freq_size - 1 + 1 + self.columns - 1)


def remote(src, dst, send, recv, **device):
    return pltpu.make_async_remote_copy(
        src_ref=src, dst_ref=dst, send_sem=send, recv_sem=recv, device_id=device, device_id_type=MESH
    )


def rows_of(index, rows):
    return pl.ds(pl.multiple_of(index * rows, rows), rows)


def series_kernel(
    sizes, direct, onsets, left_hbm, right_hbm, forward_mask, adjoint_mask, order, back, forward_table,
    inverse_table, kept, left, right, start, spectrum, got, own, ahead, total, outgoing, pair_out, pair_in,
    col_out, col_in, basis_sem, start_sem, to_send, to_recv, home_sem, sib_send, sib_recv, ring_send,
    ring_recv, relay_send, relay_recv, pair_send, pair_recv, col_send, col_recv, ret_send, ret_recv, ret_home,
):
    freq_size, pts_size, stages, rows, lines = sizes
    at = Places(freq_size, pts_size)
    freq_here, tiles = left.shape[0], left.shape[1]
    inner = freq_here // stages
    block = freq_size * rows
    spreads = {count: block_mask(tiles, lines, count) for count in {1, 2, pts_size}}
    moments = lax.broadcasted_iota(jnp.int32, (NT, NB), 0)

    def start_copy(j):
        return pltpu.make_async_copy(
            direct.at[:, pl.ds(pl.multiple_of(j * NB, NB), NB)], start.at[j], start_sem.at[j]
        )

    def basis_copies(f):
        return [
            pltpu.make_async_copy(right_hbm.at[f], right.at[f], basis_sem.at[0, f]),
            pltpu.make_async_copy(left_hbm.at[f], left.at[f], basis_sem.at[1, f]),
        ]

    def to_copy(h, j, step, adjoint):
        peer = at.freq_peer(step)
        target = own.at[h, j] if adjoint else got.at[h, at.pts, j]
        return remote(
            spectrum.at[h, j, rows_of(peer, rows), :], target.at[rows_of(at.freq, rows), :],
            to_send.at[h, j, step], to_recv.at[h, j, step], freq=peer,
        )

    def home_copy(h, j, adjoint):
        target = own.at[h, j] if adjoint else got.at[h, at.pts, j]
        return pltpu.make_async_copy(
            spectrum.at[h, j, rows_of(at.freq, rows), :], target.at[rows_of(at.freq, rows), :], home_sem.at[h, j]
        )

    def sib_copy(h, j):
        mine = got.at[h, at.pts, j]
        return remote(mine, mine, sib_send.at[h, j], sib_recv.at[h, j], pts=at.sibling())

    def ring_copy(h, j, step):
        mine = got.at[h, at.pts, j]
        return remote(
            mine, mine, ring_send.at[h, j, step], ring_recv.at[h, j, step],
            pts=at.column_peer(step) * CORES + at.core,
        )

    def relay_copy(h, j, step):
        passed = got.at[h, at.column_source(step) * CORES + at.core, j]
        return remote(
            passed, passed, relay_send.at[h, j, step], relay_recv.at[h, j, step], pts=at.sibling()
        )

    def pair_copy(h, j, step):
        return remote(
            pair_out.at[h, step, j], pair_in.at[h, step, j], pair_send.at[h, step, j],
            pair_recv.at[h, step, j], pts=at.sibling(),
        )

    def col_copy(h, j, step):
        return remote(
            col_out.at[h, step - 1, j], col_in.at[h, step - 1, j], col_send.at[h, step - 1, j],
            col_recv.at[h, step - 1, j], pts=at.column_peer(step) * CORES + at.core,
        )

    def ret_copy(h, j, step, half):
        peer = at.freq_peer(step)
        return remote(
            outgoing.at[h, j, rows_of(peer, rows), :], kept.at[half, h, j, rows_of(at.freq, rows), :],
            ret_send.at[h, j, step], ret_recv.at[h, j, step], freq=peer,
        )

    def ret_own(h, j, half):
        return pltpu.make_async_copy(
            outgoing.at[h, j, rows_of(at.freq, rows), :], kept.at[half, h, j, rows_of(at.freq, rows), :],
            ret_home.at[h, j],
        )

    def each(count, work):
        def step(j, carry):
            work(j)
            return carry

        lax.fori_loop(0, count, step, 0)

    def send_stage(h, j, adjoint):
        for step in range(1, freq_size):
            to_copy(h, j, step, adjoint).start()
        home_copy(h, j, adjoint).start()

    def send_band(j, history, adjoint):
        bands = dot_nn(forward_table[...], history).astype(bf16)
        for h in range(stages):
            spectrum[h, j] = bands[h * block : (h + 1) * block]
        send_stage(0, j, adjoint)

    def send_rest(adjoint):
        for h in range(1, stages):
            each(tiles, lambda j, h=h: send_stage(h, j, adjoint))

    def arrive(h, j, adjoint):
        for step in range(1, freq_size):
            to_copy(h, j, step, adjoint).wait_recv()
        home_copy(h, j, adjoint).wait()

    def send_back(h, j, value, half):
        outgoing[h, j] = dot_nn(back[...], value.astype(bf16)).astype(bf16)
        for step in range(1, freq_size):
            ret_copy(h, j, step, half).start()
        ret_own(h, j, half).start()

    def come_back(j, half):
        for h in range(stages):
            for step in range(1, freq_size):
                ret_copy(h, j, step, half).wait_recv()
            ret_own(h, j, half).wait()

    def turn(j, half, adjoint):
        spectra = jnp.concatenate([kept[half, h, j] for h in range(stages)], axis=0)
        field = dot_nn(inverse_table[...], spectra)
        field = jnp.where(moments < onsets[j], field, 0.0)
        send_band(j, field.astype(bf16), adjoint)

    def piece_of(value):
        return value.reshape(inner * lines, NB)

    def lines_of(j):
        return pl.ds(pl.multiple_of(j * lines, lines), lines)

    def part(h, owner, j):
        return piece_of(total[owner, h * inner : (h + 1) * inner, lines_of(j), :])

    def line_block(ordered, f):
        return ordered[f * lines : (f + 1) * lines]

    def forward_tiles(h, owners, j):
        columns = [owner * tiles + j for owner in owners]
        ordered = [dot_nn(order[...], got[h, owner, j]).astype(bf16) for owner in owners]
        first = h * inner
        terms = [
            rank_terms(
                [
                    (line_block(x, f), right[first + f, :, c], forward_mask[c, h, f : f + 1])
                    for x, c in zip(ordered, columns)
                ]
            )
            for f in range(inner)
        ]
        for f in range(inner):
            ahead[first + f] += add_up(terms[f], spreads[len(owners)], [left[first + f, :, c] for c in columns])

    def forward_stages(half):
        count = stages * tiles

        def advance(t):
            @pl.when(t < count)
            def _():
                h, j = t // tiles, t % tiles
                arrive(h, j, False)
                for step in range(1, at.columns):
                    ring_copy(h, j, step).start()
                sib_copy(h, j).start()

            @pl.when((t >= RING_LAG) & (t < count + RING_LAG))
            def _():
                m = t - RING_LAG
                h, j = m // tiles, m % tiles
                for step in range(1, at.columns):
                    ring_copy(h, j, step).wait_recv()
                    relay_copy(h, j, step).start()

            @pl.when(t >= TILE_LAG)
            def _():
                m = t - TILE_LAG
                h, j = m // tiles, m % tiles
                sib_copy(h, j).wait_recv()
                owners = [at.pts, at.sibling()]
                for step in range(1, at.columns):
                    relay_copy(h, j, step).wait_recv()
                    source = at.column_source(step) * CORES
                    owners += [source + at.core, source + 1 - at.core]
                forward_tiles(h, owners, j)

            for h in range(stages):

                @pl.when(t == TILE_LAG + (h + 1) * tiles - 1)
                def _(h=h):
                    def back_now(j):
                        value = ahead[h * inner : (h + 1) * inner, lines_of(j), :]
                        send_back(h, j, piece_of(value), half)

                    each(tiles, back_now)

        each(count + TILE_LAG, advance)

    def adjoint_tiles(h, indices):
        for j in indices:
            arrive(h, j, True)
        ordered = [dot_nn(order[...], own[h, j]).astype(bf16) for j in indices]
        first = h * inner

        spread = spreads[len(indices)]

        def group(number):
            owners = [number * CORES + core for core in range(CORES)]
            spans = [pl.ds(owner * tiles, tiles) for owner in owners]
            terms = [
                rank_terms(
                    [
                        (
                            line_block(x, f),
                            left[first + f, j, span],
                            adjoint_mask[j, owner, first + f : first + f + 1],
                        )
                        for x, j in zip(ordered, indices)
                    ]
                )
                for owner, span in zip(owners, spans)
                for f in range(inner)
            ]
            for n, (owner, span) in enumerate(zip(owners, spans)):
                for f in range(inner):
                    bases = [right[first + f, j, span] for j in indices]
                    total[owner, first + f] += add_up(terms[n * inner + f], spread, bases)

        each(at.columns, group)

    def adjoint_stage(h, half):
        pairs = tiles // 2

        def two(n):
            adjoint_tiles(h, (2 * n, 2 * n + 1))
            if h:
                close(h - 1, 2 * n, half)
                close(h - 1, 2 * n + 1, half)

        each(pairs, two)
        if tiles % 2:
            adjoint_tiles(h, (tiles - 1,))
            if h:
                close(h - 1, tiles - 1, half)

    def reduce_start(h):
        for step in list(range(1, at.columns)) + [0]:

            def pair_start(j, step=step):
                owner = at.column_peer(step) * CORES + 1 - at.core
                pair_out[h, step, j] = part(h, owner, j).astype(bf16)
                pair_copy(h, j, step).start()

            each(tiles, pair_start)
        for step in range(1, at.columns):

            def col_start(j, step=step):
                pair_copy(h, j, step).wait_recv()
                owner = at.column_peer(step) * CORES + at.core
                value = part(h, owner, j) + pair_in[h, step, j].astype(f32)
                col_out[h, step - 1, j] = value.astype(bf16)
                col_copy(h, j, step).start()

            each(tiles, col_start)

    def close(h, j, half):
        pair_copy(h, j, 0).wait_recv()
        value = part(h, at.pts, j) + pair_in[h, 0, j].astype(f32)
        for step in range(1, at.columns):
            col_copy(h, j, step).wait_recv()
            value = value + col_in[h, step - 1, j].astype(f32)
        send_back(h, j, value, half)

    def to_drain(j, adjoint):
        for h in range(stages):
            for step in range(1, freq_size):
                to_copy(h, j, step, adjoint).wait_send()

    def reduce_drain(j):
        for h in range(stages):
            for step in range(at.columns):
                pair_copy(h, j, step).wait_send()
            for step in range(1, at.columns):
                col_copy(h, j, step).wait_send()

    def gather_drain(j):
        to_drain(j, False)
        for h in range(stages):
            sib_copy(h, j).wait_send()
            for step in range(1, at.columns):
                ring_copy(h, j, step).wait_send()
                relay_copy(h, j, step).wait_send()

    def ret_drain(j, half):
        for h in range(stages):
            for step in range(1, freq_size):
                ret_copy(h, j, step, half).wait_send()

    each(tiles, lambda j: start_copy(j).start())
    for f in range(freq_here):
        for copy in basis_copies(f):
            copy.start()
    at.greet()

    def begin(j):
        start_copy(j).wait()
        send_band(j, start[j], False)

    each(tiles, begin)
    send_rest(False)
    for f in range(freq_here):
        for copy in basis_copies(f):
            copy.wait()

    def iteration(i):
        half = 2 * i
        ahead[...] = jnp.zeros_like(ahead)
        forward_stages(half)
        each(tiles, gather_drain)
        total[...] = jnp.zeros_like(total)

        def go(j):
            come_back(j, half)
            turn(j, half, True)

        each(tiles, go)
        send_rest(True)
        each(tiles, lambda j: ret_drain(j, half))
        for h in range(stages):
            adjoint_stage(h, half + 1)
            reduce_start(h)
        each(tiles, lambda j: to_drain(j, True))

        def last(t):
            @pl.when(t < tiles)
            def _():
                close(stages - 1, t, half + 1)

            @pl.when(t >= LAG)
            def _():
                come_back(t - LAG, half + 1)

            @pl.when((t >= LAG) & (i < ITERS - 1))
            def _():
                turn(t - LAG, half + 1, False)

        each(tiles + LAG, last)

        @pl.when(i < ITERS - 1)
        def _():
            send_rest(False)

        each(tiles, lambda j: ret_drain(j, half + 1))
        each(tiles, reduce_drain)

    each(ITERS, iteration)


def series_call(sizes, direct, onsets, left, right, forward_mask, adjoint_mask, order, back, forward_table, inverse_table):
    freq_size, pts_size, stages, rows, lines = sizes
    freq_here, tiles = left.shape[:2]
    block = freq_size * rows
    columns = pts_size // CORES
    dma = pltpu.SemaphoreType.DMA
    piece = (tiles, block, NB)
    scratch = [
        pltpu.VMEM(left.shape, bf16),
        pltpu.VMEM(right.shape, bf16),
        pltpu.VMEM((tiles, NT, NB), bf16),
        pltpu.VMEM((stages,) + piece, bf16),
        pltpu.VMEM((stages, pts_size) + piece, bf16),
        pltpu.VMEM((stages,) + piece, bf16),
        pltpu.VMEM((freq_here, tiles * lines, NB), f32),
        pltpu.VMEM((pts_size, freq_here, tiles * lines, NB), f32),
        pltpu.VMEM((stages,) + piece, bf16),
        pltpu.VMEM((stages, columns) + piece, bf16),
        pltpu.VMEM((stages, columns) + piece, bf16),
        pltpu.VMEM((stages, columns - 1) + piece, bf16),
        pltpu.VMEM((stages, columns - 1) + piece, bf16),
        dma((2, freq_here)),
        dma((tiles,)),
        dma((stages, tiles, freq_size)),
        dma((stages, tiles, freq_size)),
        dma((stages, tiles)),
        dma((stages, tiles)),
        dma((stages, tiles)),
        dma((stages, tiles, columns)),
        dma((stages, tiles, columns)),
        dma((stages, tiles, columns)),
        dma((stages, tiles, columns)),
        dma((stages, columns, tiles)),
        dma((stages, columns, tiles)),
        dma((stages, columns - 1, tiles)),
        dma((stages, columns - 1, tiles)),
        dma((stages, tiles, freq_size)),
        dma((stages, tiles, freq_size)),
        dma((stages, tiles)),
    ]
    vmem = pl.BlockSpec(memory_space=pltpu.VMEM)
    hbm = pl.BlockSpec(memory_space=pl.ANY)
    return pl.pallas_call(
        functools.partial(series_kernel, sizes),
        out_shape=jax.ShapeDtypeStruct((2 * ITERS, stages) + piece, bf16),
        name="series",
        in_specs=[hbm, vmem, hbm, hbm] + [vmem] * 6,
        out_specs=vmem,
        scratch_shapes=scratch,
        compiler_params=pltpu.CompilerParams(
            collective_id=1, has_side_effects=True, vmem_limit_bytes=67043328
        ),
    )(direct, onsets, left, right, forward_mask, adjoint_mask, order, back, forward_table, inverse_table)


def fields_kernel(kept, direct, onsets, inverse_table, plus, minus):
    moments = lax.broadcasted_iota(jnp.int32, (NT, NB), 0)
    inside = moments < onsets[0]

    def total(first):
        spectra = jnp.concatenate(
            [kept[half, h, 0] for half in range(first, 2 * ITERS, 2) for h in range(kept.shape[1])], axis=0
        )
        value = dot_nn(inverse_table[...], spectra)
        return jnp.where(inside, value, 0.0)

    minus[...] = total(0)
    plus[...] = direct[...].astype(f32) + total(1)


def fields_call(kept, direct, onsets, inverse_table):
    stages, tiles, block = kept.shape[1:4]
    field = pl.BlockSpec((NT, NB), lambda j: (0, j))
    return pl.pallas_call(
        fields_kernel,
        grid=(tiles,),
        out_shape=[jax.ShapeDtypeStruct(direct.shape, f32)] * 2,
        name="fields",
        in_specs=[
            pl.BlockSpec((2 * ITERS, stages, 1, block, NB), lambda j: (0, 0, j, 0, 0)),
            field,
            pl.BlockSpec((1, 1, NB), lambda j: (j, 0, 0)),
            pl.BlockSpec((NT, ITERS * stages * block), lambda j: (0, 0)),
        ],
        out_specs=[field, field],
    )(kept, direct, onsets, inverse_table)


def body(freq_size, pts_size, direct, onsets, left_bases, right_bases, tile_ranks):
    point_here, _, cells_here = direct.shape
    assert point_here == 1
    freq_here, tiles, tile_count = left_bases.shape[:3]
    points = point_here * freq_size
    lines = 2 * points
    stages = 2 if freq_here % 16 == 0 else 1
    inner = freq_here // stages
    rows = inner * 2
    block = freq_size * rows
    sizes = (freq_size, pts_size, stages, rows, lines)
    forward_table, inverse_table = band_tables(F, NT, freq_size, stages)
    inverse_table = np.ascontiguousarray(inverse_table.T)
    rank_index = lax.broadcasted_iota(jnp.int32, tile_ranks.shape + (2, K), 4)
    rank_mask = (rank_index < tile_ranks[..., None, None]).astype(f32)
    forward_mask = rank_mask.transpose(2, 0, 1, 3, 4).reshape(tile_count, stages, inner, tiles * 2 * K)
    adjoint_mask = rank_mask.transpose(1, 2, 0, 3, 4).reshape(tiles, pts_size, tiles, freq_here, 2 * K)
    adjoint_mask = adjoint_mask.transpose(0, 1, 3, 2, 4).reshape(tiles, pts_size, freq_here, tiles * 2 * K)
    left = left_bases.reshape(freq_here, tiles, tile_count, 2 * K, NB)
    right = right_bases.reshape(freq_here, tiles, tile_count, 2 * K, NB)
    old = np.arange(block)
    order = np.zeros((block, block), np.float32)
    order[old % rows * points + old // rows, old] = 1.0
    order = order.astype(bf16)
    back = np.ascontiguousarray(order.T)
    onsets = onsets.reshape(tiles, 1, NB)
    kept = series_call(
        sizes, direct[0], onsets, left, right, forward_mask, adjoint_mask, order, back, forward_table, inverse_table
    )
    plus_field, minus_field = fields_call(kept, direct[0], onsets, np.concatenate([inverse_table] * ITERS, axis=1))
    return (plus_field[None], minus_field[None])


def solution(mesh):
    return jax.shard_map(
        functools.partial(body, mesh.shape["freq"], mesh.shape["pts"]),
        mesh=mesh,
        in_specs=(
            P("freq", None, "pts"),
            P("freq", "pts"),
            P("freq", "pts", None, None, None, None),
            P("freq", "pts", None, None, None, None),
            P("freq", "pts", None),
        ),
        out_specs=(P("freq", None, "pts"), P("freq", None, "pts")),
        check_vma=False,
    )
```
